32 devices in a mesh: row: 8 (over y, x, core), col: 4 (over z).
Axes of the slice: x: 2, y: 2, z: 4, core: 2. Of those that a mesh axis runs over, the one named last changes fastest.
Arguments:
- row_cells: int32 [3, 8192], P(None, 'row'), may hold values from 0 to 63
- col_cells: int32 [3, 32768], P(None, 'col'), may hold values from 0 to 63
- omega: float32 [16, 32768], P(None, 'col'), may hold values from -6 to 6
Outputs:
- basis: float32 [16, 8192], P(None, 'row')
- image: float32 [16, 32768], P(None, 'col')
- core: float32 [16, 16], replicated
The draws below stay inside these ranges and needn't reach their ends.
All inputs are finite; a program needn't handle non-finite values.
Results may differ from the reference program's by a relative error of at most 0.0001.
Values sent between devices are 32-bit elements; how exact they have to be, the bound alone decides.
A program may use at most 64 MiB of HBM per device.

```python
import math
import jax
import jax.numpy as jnp
from jax import lax

RANK = 16
GRID = 64
ROWS = 8192
ORDER = 32768


def plant(array, rng, least, top_value):
    index_at = [jax.random.randint(jax.random.fold_in(rng, axis), (), 0, length) for axis, length in enumerate(array.shape)]
    longest = array.shape.index(max(array.shape))
    neighbour = index_at[:longest] + [(index_at[longest] + 1) % array.shape[longest]] + index_at[longest + 1:]
    return array.at[tuple(index_at)].set(least).at[tuple(neighbour)].set(top_value)


def level_of(key, extent, cuts, low, high):
    level, own = 1.0, jax.random.fold_in(key, 6)
    for position, blocks in cuts:
        draws = jnp.exp(jax.random.uniform(jax.random.fold_in(own, position), (blocks,), jnp.float32, low / len(cuts), high / len(cuts)))
        level = level * jnp.repeat(draws, extent[position] // blocks).reshape([-1 if axis == position else 1 for axis in range(len(extent))])
    return level


def noise(stream_key, extent, deviation, limit, cuts=(), dtype=jnp.bfloat16):
    factor_of = level_of(stream_key, extent, cuts, -0.22, 0.18) if cuts else 1.0
    values = jax.random.normal(stream_key, extent, jnp.float32) * deviation * factor_of
    return jnp.minimum(jnp.maximum(values, -limit), limit).astype(dtype)


def setup_inputs(seed: int = 0) -> dict:
    splits = jax.random.split(jax.random.key(seed), 4)
    return {
        "row_cells": plant(jax.random.randint(splits[0], (3, ROWS), 0, GRID), jax.random.fold_in(splits[0], 1), 0, GRID - 1).astype(jnp.int32),
        "col_cells": plant(jax.random.randint(splits[1], (3, ORDER), 0, GRID), jax.random.fold_in(splits[1], 1), 0, GRID - 1).astype(jnp.int32),
        "omega": noise(splits[2], (RANK, ORDER), 1.0, 6.0, ((1, 4),), jnp.float32),
    }


def kernel_tile(rows, cols):
    first = (rows[0][:, None] - cols[0][None, :]).astype(jnp.float32)
    total = first * first
    second = (rows[1][:, None] - cols[1][None, :]).astype(jnp.float32)
    total = total + second * second
    third = (rows[2][:, None] - cols[2][None, :]).astype(jnp.float32)
    total = total + third * third
    return 0.25 * jnp.exp(-jnp.sqrt(total) / 6.4)

def reference(row_cells, col_cells, omega):
    rows_total = row_cells.shape[1]
    order = col_cells.shape[1]
    rank = omega.shape[0]
    block = math.gcd(rows_total, 512)
    count = rows_total // block
    row_blocks = row_cells.reshape(3, count, block).transpose(1, 0, 2)

    def sketch_block(cells):
        tile = kernel_tile(cells, col_cells)
        return lax.dot_general(omega, tile, (((1,), (1,)), ((), ())), precision=lax.Precision.HIGHEST)
    parts = lax.map(sketch_block, row_blocks)
    sketch = parts.transpose(1, 0, 2).reshape(rank, rows_total)
    gram = jnp.dot(sketch, sketch.T, precision=lax.Precision.HIGHEST) / rows_total
    lower = jnp.linalg.cholesky(gram)
    basis = jax.scipy.linalg.solve_triangular(lower, sketch, lower=True)
    basis_blocks = basis.reshape(rank, count, block).transpose(1, 0, 2)

    def image_step(carry, pair):
        cells, left = pair
        tile = kernel_tile(cells, col_cells)
        return (carry + jnp.dot(left, tile, precision=lax.Precision.HIGHEST), None)
    image, _ = lax.scan(image_step, jnp.zeros((rank, order), jnp.float32), (row_blocks, basis_blocks))
    core = jnp.dot(image, image.T, precision=lax.Precision.HIGHEST) / order
    return (basis, image, core)
```

```python
import functools
import math

import jax
import jax.numpy as jnp
from jax import lax
from jax.experimental import pallas as pl
from jax.experimental.pallas import tpu as pltpu
from jax.sharding import PartitionSpec as P

BF16, F32 = jnp.bfloat16, jnp.float32
HIGHEST = lax.Precision.HIGHEST
NT = (((1,), (1,)), ((), ()))
NN = (((1,), (0,)), ((), ()))
FEATS = 128
RATE = -math.log2(math.e) / 6.4


def split(x):
    high = x.astype(BF16)
    return high, (x - high.astype(F32)).astype(BF16)


def features(cells, extent, own):
    c0, c1, c2 = (cells[d : d + 1, :].astype(F32) for d in range(3))
    norm = c0 * c0 + c1 * c1 + c2 * c2
    top = jnp.floor(norm * (1.0 / 128.0)) * 128.0
    rest = norm - top
    one = jnp.ones_like(norm)
    if own:
        rows = [c0, c1, c2, top, rest, one, one]
    else:
        rows = [-2.0 * c0, -2.0 * c1, -2.0 * c2, one, one, top, rest]
    at = lax.broadcasted_iota(jnp.int32, (extent, norm.shape[1]), 0)
    out = jnp.zeros((extent, norm.shape[1]), F32)
    for index, row in enumerate(rows):
        out = jnp.where(at == index, row, out)
    return out


def kernel(
    shape,
    row_ref, col_ref, omega_ref,
    basis_ref, image_ref, core_ref,
    rowf, colf, om, khi, klo,
    sk_src, sk_all, sk_hl, g_src, g_all, w_src, w_all, img, c_src, c_all, d_src, d_all,
    sk_ss, sk_rs, g_ss, g_rs, w_ss, w_rs, a_ss, a_rs, f_ss, f_rs, c_ss, c_rs, d_ss, d_rs,
):
    R, C, rank, M, N, chunk, wide, rows_total, order = shape
    me = lax.axis_index("row")
    mc = lax.axis_index("col")
    half = R // 2
    sib = me + 1 - 2 * lax.rem(me, 2)
    part = N // R
    chunks = M // chunk

    def row_of(t):
        return lax.rem(me + t, R)

    def row_from(t):
        return lax.rem(me - t + R, R)

    def remote(src, dst, ss, rs, axis, peer):
        return pltpu.make_async_remote_copy(
            src_ref=src, dst_ref=dst, send_sem=ss, recv_sem=rs,
            device_id={axis: peer}, device_id_type=pl.DeviceIdType.MESH,
        )

    barrier = pltpu.get_barrier_semaphore()
    for t in range(1, R):
        pl.semaphore_signal(barrier, inc=1, device_id={"row": row_of(t)}, device_id_type=pl.DeviceIdType.MESH)
    for t in range(1, C):
        pl.semaphore_signal(
            barrier, inc=1, device_id={"col": lax.rem(mc + t, C)}, device_id_type=pl.DeviceIdType.MESH
        )

    rowf[...] = features(row_ref, FEATS, True).T.astype(BF16)
    step = min(N, 1024)
    for s in range(N // step):
        cols = pl.ds(s * step, step)
        colf[:, cols] = features(col_ref.at[:, cols], FEATS, False).astype(BF16)
        high, low = split(0.25 * omega_ref[:, cols])
        om[0:rank, cols] = high
        om[rank : 2 * rank, cols] = low

    pl.semaphore_wait(barrier, R - 1 + C - 1)

    def sketch_copy(rc, t):
        return remote(
            sk_src.at[rc], sk_all.at[mc, rc], sk_ss.at[rc, t], sk_rs.at[rc, t], "col", lax.rem(mc + t, C)
        )

    def row_chunk(rc, carry):
        rows = pl.ds(pl.multiple_of(rc * chunk, chunk), chunk)

        def col_tile(ct, acc):
            cols = pl.ds(pl.multiple_of(ct * wide, wide), wide)
            sq = lax.dot_general(rowf[rows, :], colf[:, cols], NN, preferred_element_type=F32)
            sq = jnp.maximum(sq, 1e-30)
            value = jnp.exp2((sq * RATE) * lax.rsqrt(sq))
            high, low = split(value)
            khi[rows, cols] = high
            klo[rows, cols] = low
            o = om[:, cols]
            return (
                acc
                + lax.dot_general(o, high, NT, preferred_element_type=F32)
                + lax.dot_general(o, low, NT, preferred_element_type=F32)
            )

        acc = lax.fori_loop(0, N // wide, col_tile, jnp.zeros((2 * rank, chunk), F32))
        total = acc[:rank] + acc[rank:]
        sk_src[rc] = total
        sk_all[mc, rc] = total
        for t in range(1, C):
            sketch_copy(rc, t).start()
        return carry

    lax.fori_loop(0, chunks, row_chunk, 0)

    for rc in range(chunks):
        for t in range(1, C):
            sketch_copy(rc, t).wait_recv()
    pieces = []
    for rc in range(chunks):
        total = sk_all[0, rc]
        for c in range(1, C):
            total = total + sk_all[c, rc]
        pieces.append(total)
    sketch = jnp.concatenate(pieces, axis=1)
    high, low = split(0.25 * sketch)
    sk_hl[0:rank, :] = high
    sk_hl[rank : 2 * rank, :] = low
    gram = lax.dot_general(sketch, sketch, NT, precision=HIGHEST, preferred_element_type=F32) / rows_total
    g_src[...] = jnp.zeros_like(g_src)
    g_src[:, rank : 2 * rank] = gram
    g_all[me] = g_src[...]

    def gram_copy(t):
        return remote(g_src, g_all.at[me], g_ss.at[t], g_rs.at[t], "row", row_of(t))

    for t in range(1, R):
        gram_copy(t).start()

    def w_copy(t):
        return remote(w_src.at[t], w_all.at[me], w_ss.at[t], w_rs.at[t], "row", row_of(t))

    def product(peer):
        cols = pl.ds(pl.multiple_of(peer * part, part), part)
        s = sk_hl[...]
        acc = lax.dot_general(s, khi[:, cols], NN, preferred_element_type=F32)
        acc = acc + lax.dot_general(s, klo[:, cols], NN, preferred_element_type=F32)
        return acc[:rank] + acc[rank:]

    def block(t, carry):
        w_src[t] = product(row_of(t))
        w_copy(t).start()
        return carry

    lax.fori_loop(1, R, block, 0)
    w_all[me] = product(me)

    for t in range(1, R):
        gram_copy(t).wait_recv()
    mat = g_all[0]
    for r in range(1, R):
        mat = mat + g_all[r]
    sub = lax.broadcasted_iota(jnp.int32, mat.shape, 0)
    lane = lax.broadcasted_iota(jnp.int32, mat.shape, 1)
    mat = mat + jnp.where(lane == sub, 1.0, 0.0)
    for k in range(rank - 1):
        row = mat[k : k + 1, :]
        factor = mat[:, rank + k : rank + k + 1] * (1.0 / mat[k : k + 1, rank + k : rank + k + 1])
        mat = mat - jnp.where(sub > k, factor * row, 0.0)
    diag = jnp.sum(jnp.where(lane == sub + rank, mat, 0.0), axis=1, keepdims=True)
    inverse = (mat * (1.0 / jnp.sqrt(diag)))[:, :rank]
    inverse = jnp.where(lane[:, :rank] <= sub[:, :rank], inverse, 0.0)
    basis_ref[...] = jnp.dot(inverse, sketch, precision=HIGHEST, preferred_element_type=F32)

    for t in range(1, R):
        w_copy(t).wait_recv()
    total = w_all[0]
    for r in range(1, R):
        total = total + w_all[r]
    mine = jnp.dot(inverse, total, precision=HIGHEST, preferred_element_type=F32)
    img[me] = mine

    def far_copy(t):
        return remote(img.at[me], img.at[me], a_ss.at[t], a_rs.at[t], "row", row_of(2 * t))

    def near_copy(t):
        slot = row_from(2 * t)
        return remote(img.at[slot], img.at[slot], f_ss.at[t], f_rs.at[t], "row", sib)

    def core_copy(t):
        return remote(c_src, c_all.at[me], c_ss.at[t], c_rs.at[t], "row", row_of(t))

    def last_copy(t):
        return remote(d_src, d_all.at[mc], d_ss.at[t], d_rs.at[t], "col", lax.rem(mc + t, C))

    core = lax.dot_general(mine, mine, NT, precision=HIGHEST, preferred_element_type=F32) / order
    c_src[...] = jnp.zeros_like(c_src)
    c_src[:, 0:rank] = core
    c_all[me] = c_src[...]
    for t in range(1, R):
        core_copy(t).start()
    for t in range(half - 1, 0, -1):
        far_copy(t).start()
    near_copy(0).start()
    for t in range(1, R):
        core_copy(t).wait_recv()
    core = c_all[0]
    for r in range(1, R):
        core = core + c_all[r]
    d_src[...] = core
    d_all[mc] = core
    for t in range(1, C):
        last_copy(t).start()
    for t in range(1, half):
        far_copy(t).wait_recv()
        near_copy(t).start()
    for t in range(half):
        near_copy(t).wait_recv()
    for r in range(R):
        image_ref[:, r * part : (r + 1) * part] = img[r]
    for t in range(1, C):
        last_copy(t).wait_recv()
    core = d_all[0]
    for c in range(1, C):
        core = core + d_all[c]
    core_ref[...] = core[:, 0:rank]

    for rc in range(chunks):
        for t in range(1, C):
            sketch_copy(rc, t).wait_send()
    for t in range(1, R):
        gram_copy(t).wait_send()
        w_copy(t).wait_send()
        core_copy(t).wait_send()
    for t in range(1, half):
        far_copy(t).wait_send()
    for t in range(half):
        near_copy(t).wait_send()
    for t in range(1, C):
        last_copy(t).wait_send()


def shards(row_cells, col_cells, omega):
    R, C = lax.axis_size("row"), lax.axis_size("col")
    rank = omega.shape[0]
    M, N = row_cells.shape[1], col_cells.shape[1]
    chunk, wide = min(M, 256), min(N, 1024)
    chunks, part = M // chunk, N // R
    shape = (R, C, rank, M, N, chunk, wide, M * R, N * C)
    lanes = 128
    vmem = pltpu.VMEM
    dma = pltpu.SemaphoreType.DMA
    full = pl.BlockSpec(memory_space=pltpu.VMEM)
    return pl.pallas_call(
        functools.partial(kernel, shape),
        out_shape=(
            jax.ShapeDtypeStruct((rank, M), F32),
            jax.ShapeDtypeStruct((rank, N), F32),
            jax.ShapeDtypeStruct((rank, rank), F32),
        ),
        in_specs=[full] * 3,
        out_specs=(full,) * 3,
        scratch_shapes=[
            vmem((M, FEATS), BF16),
            vmem((FEATS, N), BF16),
            vmem((2 * rank, N), BF16),
            vmem((M, N), BF16),
            vmem((M, N), BF16),
            vmem((chunks, rank, chunk), F32),
            vmem((C, chunks, rank, chunk), F32),
            vmem((2 * rank, M), BF16),
            vmem((rank, lanes), F32),
            vmem((R, rank, lanes), F32),
            vmem((R, rank, part), F32),
            vmem((R, rank, part), F32),
            vmem((R, rank, part), F32),
            vmem((rank, lanes), F32),
            vmem((R, rank, lanes), F32),
            vmem((rank, lanes), F32),
            vmem((C, rank, lanes), F32),
            dma((chunks, C)), dma((chunks, C)),
            dma((R,)), dma((R,)),
            dma((R,)), dma((R,)),
            dma((R,)), dma((R,)),
            dma((R,)), dma((R,)),
            dma((R,)), dma((R,)),
            dma((C,)), dma((C,)),
        ],
        compiler_params=pltpu.CompilerParams(
            collective_id=0, has_side_effects=True, vmem_limit_bytes=60 * 1024 * 1024
        ),
    )(row_cells, col_cells, omega)


def solution(mesh):
    return jax.shard_map(
        shards,
        mesh=mesh,
        in_specs=(P(None, "row"), P(None, "col"), P(None, "col")),
        out_specs=(P(None, "row"), P(None, "col"), P()),
        check_vma=False,
    )
```

```python
import functools
import math

import jax
import jax.numpy as jnp
from jax import lax
from jax.experimental import pallas as pl
from jax.experimental.pallas import tpu as pltpu
from jax.sharding import PartitionSpec as P

BF16, F32 = jnp.bfloat16, jnp.float32
HIGHEST = lax.Precision.HIGHEST
NT = (((1,), (1,)), ((), ()))
NN = (((1,), (0,)), ((), ()))
LANES = 128
RATE = -math.log2(math.e) / 6.4


def split(x):
    high = x.astype(BF16)
    return high, (x - high.astype(F32)).astype(BF16)


def kernel(
    shape,
    row_ref, col_ref, omega_ref,
    basis_ref, image_ref, core_ref,
    rowb, colc, om, khi, klo,
    sk_src, sk_all, sk_hl, g_src, g_all, w_src, w_all, img, c_src, c_all, d_src, d_all,
    sk_ss, sk_rs, g_ss, g_rs, w_ss, w_rs, a_ss, a_rs, f_ss, f_rs, c_ss, c_rs, d_ss, d_rs,
):
    R, C, rank, M, N, chunk, wide, rows_total, order = shape
    me = lax.axis_index("row")
    mc = lax.axis_index("col")
    half = R // 2
    sib = me + 1 - 2 * lax.rem(me, 2)
    part = N // R
    chunks = M // chunk

    def row_of(t):
        return lax.rem(me + t, R)

    def row_from(t):
        return lax.rem(me - t + R, R)

    def remote(src, dst, ss, rs, axis, peer):
        return pltpu.make_async_remote_copy(
            src_ref=src, dst_ref=dst, send_sem=ss, recv_sem=rs,
            device_id={axis: peer}, device_id_type=pl.DeviceIdType.MESH,
        )

    barrier = pltpu.get_barrier_semaphore()
    for t in range(1, R):
        pl.semaphore_signal(barrier, inc=1, device_id={"row": row_of(t)}, device_id_type=pl.DeviceIdType.MESH)
    for t in range(1, C):
        pl.semaphore_signal(
            barrier, inc=1, device_id={"col": lax.rem(mc + t, C)}, device_id_type=pl.DeviceIdType.MESH
        )

    for d in range(3):
        rowb[d] = jnp.broadcast_to(row_ref[d : d + 1, :].astype(F32), (LANES, M)).T
    step = min(N, 1024)
    for s in range(N // step):
        cols = pl.ds(s * step, step)
        colc[0:3, cols] = col_ref[:, cols].astype(F32)
        high, low = split(0.25 * omega_ref[:, cols])
        om[0:rank, cols] = high
        om[rank : 2 * rank, cols] = low

    pl.semaphore_wait(barrier, R - 1 + C - 1)

    def sketch_copy(rc, t):
        return remote(
            sk_src.at[rc], sk_all.at[mc, rc], sk_ss.at[rc, t], sk_rs.at[rc, t], "col", lax.rem(mc + t, C)
        )

    def row_chunk(rc, carry):
        rows = pl.ds(pl.multiple_of(rc * chunk, chunk), chunk)

        def col_tile(ct, acc):
            cols = pl.ds(pl.multiple_of(ct * wide, wide), wide)
            repeat = (1, wide // LANES)
            sq = None
            for d in range(3):
                gap = jnp.tile(rowb[d, rows, :], repeat) - colc[d : d + 1, cols]
                sq = gap * gap if sq is None else sq + gap * gap
            sq = jnp.maximum(sq, 1e-30)
            value = jnp.exp2((sq * RATE) * lax.rsqrt(sq))
            high, low = split(value)
            khi[rows, cols] = high
            klo[rows, cols] = low
            o = om[:, cols]
            return (
                acc
                + lax.dot_general(o, high, NT, preferred_element_type=F32)
                + lax.dot_general(o, low, NT, preferred_element_type=F32)
            )

        acc = lax.fori_loop(0, N // wide, col_tile, jnp.zeros((2 * rank, chunk), F32))
        total = acc[:rank] + acc[rank:]
        sk_src[rc] = total
        sk_all[mc, rc] = total
        for t in range(1, C):
            sketch_copy(rc, t).start()
        return carry

    lax.fori_loop(0, chunks, row_chunk, 0)

    for rc in range(chunks):
        for t in range(1, C):
            sketch_copy(rc, t).wait_recv()
    pieces = []
    for rc in range(chunks):
        total = sk_all[0, rc]
        for c in range(1, C):
            total = total + sk_all[c, rc]
        pieces.append(total)
    sketch = jnp.concatenate(pieces, axis=1)
    high, low = split(0.25 * sketch)
    sk_hl[0:rank, :] = high
    sk_hl[rank : 2 * rank, :] = low
    gram = lax.dot_general(sketch, sketch, NT, precision=HIGHEST, preferred_element_type=F32) / rows_total
    g_src[...] = jnp.zeros_like(g_src)
    g_src[:, rank : 2 * rank] = gram
    g_all[me] = g_src[...]

    def gram_copy(t):
        return remote(g_src, g_all.at[me], g_ss.at[t], g_rs.at[t], "row", row_of(t))

    for t in range(1, R):
        gram_copy(t).start()

    def w_copy(t):
        return remote(w_src.at[t], w_all.at[me], w_ss.at[t], w_rs.at[t], "row", row_of(t))

    def product(peer):
        cols = pl.ds(pl.multiple_of(peer * part, part), part)
        s = sk_hl[...]
        acc = lax.dot_general(s, khi[:, cols], NN, preferred_element_type=F32)
        acc = acc + lax.dot_general(s, klo[:, cols], NN, preferred_element_type=F32)
        return acc[:rank] + acc[rank:]

    def block(t, carry):
        w_src[t] = product(row_of(t))
        w_copy(t).start()
        return carry

    lax.fori_loop(1, R, block, 0)
    w_all[me] = product(me)

    for t in range(1, R):
        gram_copy(t).wait_recv()
    mat = g_all[0]
    for r in range(1, R):
        mat = mat + g_all[r]
    sub = lax.broadcasted_iota(jnp.int32, mat.shape, 0)
    lane = lax.broadcasted_iota(jnp.int32, mat.shape, 1)
    mat = mat + jnp.where(lane == sub, 1.0, 0.0)
    for k in range(rank - 1):
        row = mat[k : k + 1, :]
        factor = mat[:, rank + k : rank + k + 1] * (1.0 / mat[k : k + 1, rank + k : rank + k + 1])
        mat = mat - jnp.where(sub > k, factor * row, 0.0)
    diag = jnp.sum(jnp.where(lane == sub + rank, mat, 0.0), axis=1, keepdims=True)
    inverse = (mat * (1.0 / jnp.sqrt(diag)))[:, :rank]
    inverse = jnp.where(lane[:, :rank] <= sub[:, :rank], inverse, 0.0)
    basis_ref[...] = jnp.dot(inverse, sketch, precision=HIGHEST, preferred_element_type=F32)

    for t in range(1, R):
        w_copy(t).wait_recv()
    total = w_all[0]
    for r in range(1, R):
        total = total + w_all[r]
    mine = jnp.dot(inverse, total, precision=HIGHEST, preferred_element_type=F32)
    img[me] = mine

    def far_copy(t):
        return remote(img.at[me], img.at[me], a_ss.at[t], a_rs.at[t], "row", row_of(2 * t))

    def near_copy(t):
        slot = row_from(2 * t)
        return remote(img.at[slot], img.at[slot], f_ss.at[t], f_rs.at[t], "row", sib)

    def core_copy(t):
        return remote(c_src, c_all.at[me], c_ss.at[t], c_rs.at[t], "row", row_of(t))

    def last_copy(t):
        return remote(d_src, d_all.at[mc], d_ss.at[t], d_rs.at[t], "col", lax.rem(mc + t, C))

    core = lax.dot_general(mine, mine, NT, precision=HIGHEST, preferred_element_type=F32) / order
    c_src[...] = jnp.zeros_like(c_src)
    c_src[:, 0:rank] = core
    c_all[me] = c_src[...]
    for t in range(1, R):
        core_copy(t).start()
    for t in range(half - 1, 0, -1):
        far_copy(t).start()
    near_copy(0).start()
    for t in range(1, R):
        core_copy(t).wait_recv()
    core = c_all[0]
    for r in range(1, R):
        core = core + c_all[r]
    d_src[...] = core
    d_all[mc] = core
    for t in range(1, C):
        last_copy(t).start()
    for t in range(1, half):
        far_copy(t).wait_recv()
        near_copy(t).start()
    for t in range(half):
        near_copy(t).wait_recv()
    for r in range(R):
        image_ref[:, r * part : (r + 1) * part] = img[r]
    for t in range(1, C):
        last_copy(t).wait_recv()
    core = d_all[0]
    for c in range(1, C):
        core = core + d_all[c]
    core_ref[...] = core[:, 0:rank]

    for rc in range(chunks):
        for t in range(1, C):
            sketch_copy(rc, t).wait_send()
    for t in range(1, R):
        gram_copy(t).wait_send()
        w_copy(t).wait_send()
        core_copy(t).wait_send()
    for t in range(1, half):
        far_copy(t).wait_send()
    for t in range(half):
        near_copy(t).wait_send()
    for t in range(1, C):
        last_copy(t).wait_send()


def finish(*refs):
    for source, target in zip(refs[:3], refs[3:]):
        target[...] = source[...]


def shards(row_cells, col_cells, omega):
    R, C = lax.axis_size("row"), lax.axis_size("col")
    rank = omega.shape[0]
    M, N = row_cells.shape[1], col_cells.shape[1]
    chunk, wide = min(M, 256), min(N, 1024)
    chunks, part = M // chunk, N // R
    shape = (R, C, rank, M, N, chunk, wide, M * R, N * C)
    vmem = pltpu.VMEM
    dma = pltpu.SemaphoreType.DMA
    full = pl.BlockSpec(memory_space=pltpu.VMEM)
    out_shape = (
        jax.ShapeDtypeStruct((rank, M), F32),
        jax.ShapeDtypeStruct((rank, N), F32),
        jax.ShapeDtypeStruct((rank, rank), F32),
    )
    outs = pl.pallas_call(
        functools.partial(kernel, shape),
        out_shape=out_shape,
        in_specs=[full] * 3,
        out_specs=(full,) * 3,
        scratch_shapes=[
            vmem((3, M, LANES), F32),
            vmem((8, N), F32),
            vmem((2 * rank, N), BF16),
            vmem((M, N), BF16),
            vmem((M, N), BF16),
            vmem((chunks, rank, chunk), F32),
            vmem((C, chunks, rank, chunk), F32),
            vmem((2 * rank, M), BF16),
            vmem((rank, LANES), F32),
            vmem((R, rank, LANES), F32),
            vmem((R, rank, part), F32),
            vmem((R, rank, part), F32),
            vmem((R, rank, part), F32),
            vmem((rank, LANES), F32),
            vmem((R, rank, LANES), F32),
            vmem((rank, LANES), F32),
            vmem((C, rank, LANES), F32),
            dma((chunks, C)), dma((chunks, C)),
            dma((R,)), dma((R,)),
            dma((R,)), dma((R,)),
            dma((R,)), dma((R,)),
            dma((R,)), dma((R,)),
            dma((R,)), dma((R,)),
            dma((C,)), dma((C,)),
        ],
        compiler_params=pltpu.CompilerParams(
            collective_id=0, has_side_effects=True, vmem_limit_bytes=46 * 1024 * 1024
        ),
    )(row_cells, col_cells, omega)
    return pl.pallas_call(
        finish,
        out_shape=out_shape,
        in_specs=[full] * 3,
        out_specs=(full,) * 3,
        compiler_params=pltpu.CompilerParams(vmem_limit_bytes=4 * 1024 * 1024),
    )(*outs)


def solution(mesh):
    return jax.shard_map(
        shards,
        mesh=mesh,
        in_specs=(P(None, "row"), P(None, "col"), P(None, "col")),
        out_specs=(P(None, "row"), P(None, "col"), P()),
        check_vma=False,
    )
```
